32 devices in a mesh: blk: 16 (over z, y, core), row: 2 (over x).
Axes of the slice: x: 2, y: 2, z: 4, core: 2. Of those that a mesh axis runs over, the one named last changes fastest.
Arguments:
- features: bfloat16 [12288, 2048], P('row', 'blk'), parts along dimension 0, may hold values from -6 to 6
- link_values: bfloat16 [8, 32, 2048], P(None, None, 'blk'), may hold values from -1 to 1
- link_columns: int32 [8, 32, 2048], P(None, None, 'blk'), may hold values from 0 to 255
- layer_bias: float32 [8, 2048], P(None, 'blk'), may hold values from -0.5 to 0.5
Outputs:
- outputs: bfloat16 [12288, 2048], P('row', 'blk'), parts along dimension 0
The draws below stay inside these ranges and needn't reach their ends.
There are 2 independent parts, one for each index of `row`. The reference program is written for one: setup_inputs(seed, part) draws one part's arguments, and reference() takes and returns one part's arrays. A program takes and returns all parts, laid end to end along the dimension named above; an argument that names none is the same for every part. Nothing has to cross between parts.
All inputs are finite; a program needn't handle non-finite values.
Results may differ from the reference program's by a relative error of at most 0.0072.
Values may be sent and summed in bfloat16 or wider, within the bound.
No kernel may reach another device: no remote copies, remote signals or barrier semaphores. Data moves between devices by JAX's collectives and lax.ppermute only.
A program may use at most 64 MiB of HBM per device.

```python
import math
import jax
import jax.numpy as jnp

BLOCK = 128
FANIN = 32
LAYERS = 8
ROWS = 6144
NEURONS = 2048
N_BLK = 16


def dense_choice(key):
    block_count = NEURONS // BLOCK
    layer_keys = jax.random.split(jax.random.fold_in(key, 911), LAYERS)
    orders = jax.vmap(lambda single: jax.random.permutation(single, block_count))(layer_keys)
    chosen = orders < block_count // 4
    return jnp.repeat(chosen, BLOCK, axis=1)


def draw_layer_bias(key, part):
    chosen = dense_choice(key)
    drawn = jax.random.uniform(jax.random.fold_in(key, 17), (LAYERS, NEURONS), jnp.float32, -0.5, 0.5)
    lifted = jax.random.uniform(jax.random.fold_in(key, 23), (LAYERS, NEURONS), jnp.float32, 0.3, 0.5)
    return jnp.where(chosen, lifted, drawn).astype(jnp.float32)


def draw_link_values(key, part):
    chosen = dense_choice(key)
    spread = 1.0 / math.sqrt(FANIN // 2)
    limit = 1.0 / spread
    unscaled = jax.random.truncated_normal(jax.random.fold_in(key, 37), -limit, limit, (LAYERS, FANIN, NEURONS), jnp.float32)
    factor = jnp.where(chosen, 0.3, 1.0).astype(jnp.float32)[:, None, :]
    return (unscaled * spread * factor).astype(jnp.bfloat16)


def touch_ends(drawn, rng, least, largest):
    extent = drawn.shape
    spot = [jax.random.randint(jax.random.fold_in(rng, axis), (), 0, extent[axis]) for axis in range(len(extent))]
    drawn = drawn.at[tuple(spot)].set(least)
    longest = extent.index(max(extent))
    spot[longest] = (spot[longest] + 1) % extent[longest]
    return drawn.at[tuple(spot)].set(largest)


def levels(own_key, shape, pieces, smallest, top_value):
    loudness, own = 1.0, jax.random.fold_in(own_key, 6)
    for dim, blocks in pieces:
        draws = jnp.exp(jax.random.uniform(jax.random.fold_in(own, dim), (blocks,), jnp.float32, smallest / len(pieces), top_value / len(pieces)))
        loudness = loudness * jnp.repeat(draws, shape[dim] // blocks).reshape([-1 if axis == dim else 1 for axis in range(len(shape))])
    return loudness


def gaussian(rng, dims, deviation, bound, cuts=(), kind=jnp.bfloat16):
    result = jax.random.normal(rng, dims, jnp.float32) * deviation
    if len(cuts) > 0:
        result = levels(rng, dims, cuts, -0.22, 0.18) * result
    return jnp.clip(result, min=-bound, max=bound).astype(kind)


def setup_inputs(seed: int = 0, part: int = 0) -> dict:
    key_of = jax.random.split(jax.random.key(seed), 5)
    part_keys = jax.random.split(jax.random.fold_in(key_of[4], part), 5)
    features = gaussian(part_keys[0], (ROWS, NEURONS), 1.0, 6.0, ((1, 16),))
    link_values = draw_link_values(jax.random.fold_in(key_of[4], 71), part)
    link_columns = touch_ends(jax.random.randint(key_of[2], (LAYERS, FANIN, NEURONS), 0, 2 * BLOCK), jax.random.fold_in(key_of[2], 1), 0, (2 * BLOCK) - 1).astype(jnp.int32)
    layer_bias = draw_layer_bias(jax.random.fold_in(key_of[4], 71), part)
    return {"features": features, "link_values": link_values, "link_columns": link_columns, "layer_bias": layer_bias}


ceiling_value = 4.0


def dense_layer(values_layer, columns_layer):
    target = jnp.broadcast_to(jnp.arange(NEURONS, dtype=jnp.int32)[None, :], columns_layer.shape)
    summed = jnp.zeros((NEURONS, 2 * BLOCK), jnp.float32).at[target, columns_layer.astype(jnp.int32)].add(values_layer.astype(jnp.float32))
    weights = summed.astype(jnp.bfloat16).reshape(N_BLK, BLOCK, 2 * BLOCK)
    return jnp.transpose(weights, (0, 2, 1))


def reference(features, link_values, link_columns, layer_bias):
    bit_count = N_BLK.bit_length() - 1
    blocks = features.reshape(ROWS, N_BLK, BLOCK)
    owners = jnp.arange(N_BLK, dtype=jnp.int32)
    for layer_at in range(LAYERS):
        stride = 2 ** (layer_at % bit_count)
        weights = dense_layer(link_values[layer_at], link_columns[layer_at]).astype(jnp.float32)
        partner = blocks[:, jnp.bitwise_xor(owners, stride).astype(jnp.int32)]
        preact = jnp.einsum('rnk,nko->rno', blocks.astype(jnp.float32), weights[:, :BLOCK])
        preact = preact + jnp.einsum('rnk,nko->rno', partner.astype(jnp.float32), weights[:, BLOCK:])
        preact = preact + layer_bias[layer_at].reshape(N_BLK, BLOCK)[None, :, :]
        blocks = jnp.minimum(jnp.maximum(preact, 0.0), ceiling_value).astype(jnp.bfloat16)
    return blocks.reshape(ROWS, NEURONS)
```

```python
import functools

import jax
import jax.numpy as jnp
from jax import lax
from jax.experimental import pallas as pl
from jax.experimental.pallas import tpu as pltpu
from jax.sharding import PartitionSpec as P

LAYERS = 8
CEILING = 4.0

VMEM = pl.BlockSpec(memory_space=pltpu.VMEM)
SMEM = pl.BlockSpec(memory_space=pltpu.SMEM)
ANY = pl.BlockSpec(memory_space=pl.ANY)


def exchange(value, axis, mask):
    pairs = [(source, source ^ mask) for source in range(lax.axis_size(axis))]
    return lax.ppermute(value, axis, pairs)


def finish(preact):
    return jnp.minimum(jnp.maximum(preact, 0.0), CEILING).astype(jnp.bfloat16)


def dense_block(values_layer, columns_layer):
    block_width = values_layer.shape[1]
    columns = lax.broadcasted_iota(jnp.int32, (1, 2 * block_width, 1), 1)
    onehot = columns_layer[:, None, :] == columns
    summed = jnp.sum(jnp.where(onehot, values_layer.astype(jnp.float32)[:, None, :], 0.0), axis=0)
    return summed.astype(jnp.bfloat16)


def plain_shards(features, link_values, link_columns, layer_bias):
    block_width = features.shape[1]
    bit_count = lax.axis_size("blk").bit_length() - 1
    blocks = features
    for layer_at in range(LAYERS):
        mask = 2 ** (layer_at % bit_count)
        weights = dense_block(link_values[layer_at], link_columns[layer_at])
        half_count = blocks.shape[0] // 2
        pieces = []
        for part_at in range(2):
            half_rows = blocks[part_at * half_count : (part_at + 1) * half_count]
            partner = exchange(half_rows, "blk", mask)
            own_part = jnp.dot(half_rows, weights[:block_width], preferred_element_type=jnp.float32)
            peer_part = jnp.dot(partner, weights[block_width:], preferred_element_type=jnp.float32)
            pieces.append(finish(own_part + peer_part + layer_bias[layer_at][None, :]))
        blocks = jnp.concatenate(pieces, axis=0)
    return blocks


def scatter_columns(values, columns, width, store):
    fan = values.shape[0]
    group = 64
    for first in range(0, 2 * width, group):
        index = lax.broadcasted_iota(jnp.int32, (group, width), 0) + first
        total = jnp.zeros((group, width), jnp.float32)
        for at in range(fan):
            total = total + jnp.where(columns[at : at + 1, :] == index, values[at : at + 1, :], 0.0)
        store(first, group, total.astype(jnp.bfloat16))


def first_build_kernel(values_ref, columns_ref, dense_ref):
    width = values_ref.shape[1]

    def store(first, group, tile):
        dense_ref[first : first + group, :] = tile

    scatter_columns(values_ref[...].astype(jnp.float32), columns_ref[...], width, store)


def build_kernel(masks, bit_count, layers, half_fan, *refs):
    count = len(masks)
    ins, outs = refs[: 2 * count], refs[2 * count :]
    width = outs[0].shape[1]
    for at, mask in enumerate(masks):
        parts = ins[2 * at : 2 * at + 2]
        dense_ref, bias_ref = outs[2 * at], outs[2 * at + 1]

        @pl.loop(0, layers)
        def _(layer):
            start = pl.multiple_of(layer * half_fan, half_fan)
            base = layers * half_fan
            values = jnp.concatenate([p[pl.ds(start, half_fan), :].astype(jnp.float32) for p in parts], axis=0)
            columns = jnp.concatenate(
                [p[pl.ds(pl.multiple_of(base + start, half_fan), half_fan), :].astype(jnp.float32).astype(jnp.int32) for p in parts],
                axis=0,
            )
            bit = lax.rem(layer + 1, bit_count)
            flip = lax.shift_right_logical(mask, bit) & 1

            def store(first, group, tile):
                half = first // width
                row = layer * (2 * width) + (half ^ flip) * width + first % width
                dense_ref[pl.ds(pl.multiple_of(row, group), group), :] = tile

            scatter_columns(values, columns, width, store)

        base = 2 * layers * half_fan
        rows = parts[0][base : base + 32, :].astype(jnp.float32)
        bias_ref[...] = rows[0:8] + (rows[8:16] + rows[16:24])


def build(masks, bit_count, layers, half_fan, pairs):
    width = pairs[0][0].shape[1]
    shapes = []
    for _ in masks:
        shapes += [
            jax.ShapeDtypeStruct((layers * 2 * width, width), jnp.bfloat16),
            jax.ShapeDtypeStruct((8, width), jnp.float32),
        ]
    flat = [x for pair in pairs for x in pair]
    work = len(masks) * layers
    out = pl.pallas_call(
        functools.partial(build_kernel, masks, bit_count, layers, half_fan),
        out_shape=shapes,
        in_specs=[VMEM] * len(flat),
        out_specs=[VMEM] * len(shapes),
        compiler_params=pltpu.CompilerParams(vmem_limit_bytes=16 * 2**20),
        cost_estimate=pl.CostEstimate(flops=work * 400_000_00, bytes_accessed=work * 80_000, transcendentals=0),
        name="build",
    )(*flat)
    return [(out[2 * at], out[2 * at + 1]) for at in range(len(masks))]


def home_kernel(chunk_first, rows, group_ref, own_ref, peer_ref, dense_ref, bias_ref, *out_refs):
    group_of = group_ref[0]
    dense = dense_ref[...]
    bias = bias_ref[0:1, :]
    for at, out_ref in enumerate(out_refs):
        start = pl.multiple_of(chunk_first + (group_of ^ at) * rows, rows)
        both = jnp.concatenate([own_ref[pl.ds(start, rows), :], peer_ref[pl.ds(start, rows), :]], axis=1)
        out_ref[...] = finish(jnp.dot(both, dense, preferred_element_type=jnp.float32) + bias)


def mix(read, write, layer, flip_at, dense_refs, bias_refs):
    count = len(dense_refs)
    width = dense_refs[0].shape[1]
    depth = 2 * width
    for a in range(count):
        b = a ^ flip_at
        if a > b:
            continue
        both = jnp.concatenate([read(a), read(b)], axis=1)
        dense = jnp.concatenate([dense_refs[x][layer * depth : (layer + 1) * depth, :] for x in (a, b)], axis=1)
        bias = jnp.concatenate([bias_refs[x][layer : layer + 1, :] for x in (a, b)], axis=1)
        done = finish(jnp.dot(both, dense, preferred_element_type=jnp.float32) + bias)
        write(a, done[:, :width])
        write(b, done[:, width:])


def segment_kernel(layers, count, has_peer, split_out, *refs):
    refs = list(refs)
    take = lambda number: [refs.pop(0) for _ in range(number)]
    if has_peer:
        own_ref, peer_ref = take(2)
        read = lambda at: own_ref[at]
    else:
        piece_refs = take(count)
        read = lambda at: piece_refs[at][...]
    dense_refs, bias_refs = take(count), take(count)
    out_refs = take(count if split_out else 1)
    scratch = take(2)
    width = dense_refs[0].shape[1]
    depth = 2 * width
    for step, (layer, flip_at) in enumerate(layers):
        if step == len(layers) - 1:
            if split_out:
                write = lambda at, value: out_refs[at].__setitem__(..., value)
            else:
                write = lambda at, value: out_refs[0].__setitem__(at, value)
        else:
            write = lambda at, value, to=scratch[step % 2]: to.__setitem__(at, value)
        if flip_at == 0:
            for at in range(count):
                both = jnp.concatenate([own_ref[at], peer_ref[at]], axis=1)
                dense = dense_refs[at][layer * depth : (layer + 1) * depth, :]
                bias = bias_refs[at][layer : layer + 1, :]
                write(at, finish(jnp.dot(both, dense, preferred_element_type=jnp.float32) + bias))
        else:
            mix(read, write, layer, flip_at, dense_refs, bias_refs)
        read = lambda at, source=scratch[step % 2]: source[at]


def segment(layers, inputs, dense, bias, rows, split_out):
    count, width = len(dense), dense[0].shape[1]
    has_peer = layers[0][1] == 0
    if split_out:
        shapes = [jax.ShapeDtypeStruct((rows, width), jnp.bfloat16)] * count
    else:
        shapes = [jax.ShapeDtypeStruct((count, rows, width), jnp.bfloat16)]
    operands = list(inputs) + list(dense) + list(bias)
    flops = 4 * count * len(layers) * rows * width * width
    out = pl.pallas_call(
        functools.partial(segment_kernel, layers, count, has_peer, split_out),
        out_shape=shapes,
        in_specs=[VMEM] * len(operands),
        out_specs=[VMEM] * len(shapes),
        scratch_shapes=[pltpu.VMEM((count, rows, width), jnp.bfloat16)] * 2,
        compiler_params=pltpu.CompilerParams(vmem_limit_bytes=20 * 2**20),
        cost_estimate=pl.CostEstimate(flops=flops, bytes_accessed=4 * count * rows * width, transcendentals=0),
        name="segment",
    )(*operands)
    return out


def place_kernel(chunk_first, rows, group_ref, previous_ref, *refs):
    pieces, out_ref, sems = refs[:-2], refs[-2], refs[-1]
    group_of = group_ref[0]
    copies = []
    for at, piece in enumerate(pieces):
        start = pl.multiple_of(chunk_first + (group_of ^ at) * rows, rows)
        copies.append(pltpu.make_async_copy(piece, out_ref.at[pl.ds(start, rows), :], sems.at[at]))
    for copy in copies:
        copy.start()
    for copy in copies:
        copy.wait()


def place(chunk_first, rows, group_of, previous, pieces, shape):
    first = previous is None
    body = functools.partial(place_kernel, chunk_first, rows)
    kernel = (lambda group_ref, *refs: body(group_ref, None, *refs)) if first else body
    operands = [group_of] + ([] if first else [previous]) + list(pieces)
    return pl.pallas_call(
        kernel,
        out_shape=jax.ShapeDtypeStruct(shape, jnp.bfloat16),
        in_specs=[SMEM] + ([] if first else [ANY]) + [VMEM] * len(pieces),
        out_specs=ANY,
        scratch_shapes=[pltpu.SemaphoreType.DMA((len(pieces),))],
        input_output_aliases={} if first else {1: 0},
        compiler_params=pltpu.CompilerParams(vmem_limit_bytes=8 * 2**20),
        cost_estimate=pl.CostEstimate(flops=1_000_000, bytes_accessed=1_000_000, transcendentals=0),
        name="place",
    )(*operands)


def split_bias(bias):
    terms = []
    for _ in range(3):
        term = lax.reduce_precision(bias, exponent_bits=8, mantissa_bits=7)
        terms.append(term.astype(jnp.bfloat16))
        bias = bias - term
    return terms


def swapped_shards(swapped, features, link_values, link_columns, layer_bias):
    row_count, width = features.shape
    fan = link_values.shape[1]
    half_fan = fan // 2
    bit_count = lax.axis_size("blk").bit_length() - 1
    count = 2 ** len(swapped)
    masks = [sum(1 << bit for t, bit in enumerate(swapped) if at >> t & 1) for at in range(count)]
    place_of = {bit: 1 << t for t, bit in enumerate(swapped)}
    group_of = lax.shift_right_logical(lax.axis_index("blk"), swapped[0]).astype(jnp.int32)
    group_of = jnp.bitwise_and(group_of, count - 1)[None]
    inner = LAYERS - 1

    bias_terms = [jnp.pad(t[1:], ((0, 1), (0, 0))) for t in split_bias(layer_bias)]
    bias_rows = jnp.concatenate(bias_terms + [jnp.zeros_like(bias_terms[0])], axis=0)
    columns16 = link_columns.astype(jnp.bfloat16)

    def packed(part):
        first = part * half_fan
        cut = lambda x: lax.dynamic_slice_in_dim(x[1:], first, half_fan, axis=1).reshape(inner * half_fan, width)
        return jnp.concatenate([cut(link_values), cut(columns16), bias_rows], axis=0)

    side = lax.axis_index("row")
    mine = {0: packed(side)}
    other = {0: packed(1 - side)}

    peer_features = exchange(features, "blk", 1)

    for at in (6, 4, 2):
        mine[at] = exchange(mine[0], "blk", masks[at])

    dense0 = pl.pallas_call(
        first_build_kernel,
        out_shape=jax.ShapeDtypeStruct((2 * width, width), jnp.bfloat16),
        in_specs=[VMEM] * 2,
        out_specs=VMEM,
        compiler_params=pltpu.CompilerParams(vmem_limit_bytes=4 * 2**20),
        name="first_build",
    )(link_values[0], link_columns[0])

    chunk_count = 3
    rows = row_count // (chunk_count * count)

    sent = []
    for chunk in range(chunk_count):
        sent.append(
            pl.pallas_call(
                functools.partial(home_kernel, chunk * count * rows, rows),
                out_shape=[jax.ShapeDtypeStruct((rows, width), jnp.bfloat16)] * count,
                in_specs=[SMEM] + [VMEM] * 4,
                out_specs=[VMEM] * count,
                compiler_params=pltpu.CompilerParams(vmem_limit_bytes=16 * 2**20),
                cost_estimate=pl.CostEstimate(flops=4 * count * rows * width * width, bytes_accessed=6 * count * rows * width, transcendentals=0),
                name="home",
            )(group_of, features, peer_features, dense0, layer_bias)
        )

    def arrive(chunk):
        pieces = {0: sent[chunk][0]}
        for at in (6, 7, 4, 5, 2, 3, 1):
            pieces[at] = exchange(sent[chunk][at], "blk", masks[at])
        return [pieces[at] for at in range(count)]

    arrived = [arrive(chunk) for chunk in range(chunk_count)]

    stack = lambda xs: jnp.stack(xs, axis=0)
    over_y = exchange(stack([mine[0], mine[2], mine[4], mine[6], other[0]]), "blk", masks[1])
    over_x = exchange(stack([mine[2], mine[4], mine[6]]), "row", 1)
    for at in range(4):
        mine[1 + 2 * at] = over_y[at]
    other[1] = over_y[4]
    for at in range(3):
        other[2 + 2 * at] = over_x[at]
    last_x = exchange(over_y[1:3], "row", 1)
    last_y = exchange(over_x[2], "blk", masks[1])
    other[3], other[5] = last_x[0], last_x[1]
    other[7] = last_y

    weights = {}
    for group in ((0,), (2, 4, 6, 1), (3, 5, 7)):
        made = build([masks[at] for at in group], bit_count, inner, half_fan, [(mine[at], other[at]) for at in group])
        for at, one in zip(group, made):
            weights[at] = one
    dense = [weights[at][0] for at in range(count)]
    bias = [weights[at][1] for at in range(count)]

    segments = []
    for layer_at in range(1, LAYERS):
        bit = layer_at % bit_count
        flip = place_of.get(bit, 0)
        if flip == 0 or not segments:
            segments.append([])
        segments[-1].append((layer_at - 1, flip))

    result = None
    for chunk in range(chunk_count):
        state = arrived[chunk]
        for at, layers in enumerate(segments):
            last = at == len(segments) - 1
            out = segment(tuple(layers), state, dense, bias, rows, last)
            if last:
                state = out
            else:
                state = [out[0], exchange(out[0], "blk", 1)]
        back = {0: state[0]}
        for at in (6, 7, 4, 5, 2, 3, 1):
            back[at] = exchange(state[at], "blk", masks[at])
        pieces = [back[at] for at in range(count)]
        result = place(chunk * count * rows, rows, group_of, result, pieces, (row_count, width))
    return result


def solution(mesh):
    bit_count = mesh.shape["blk"].bit_length() - 1
    uses = [len([l for l in range(LAYERS) if l % bit_count == bit]) for bit in range(bit_count)]
    swapped = tuple(bit for bit in range(1, bit_count) if uses[bit] >= 2)
    if len(swapped) == 3 and swapped == (1, 2, 3) and mesh.shape["row"] == 2:
        body = functools.partial(swapped_shards, swapped)
    else:
        body = plain_shards
    return jax.shard_map(
        body,
        mesh=mesh,
        in_specs=(P("row", "blk"), P(None, None, "blk"), P(None, None, "blk"), P(None, "blk")),
        out_specs=P("row", "blk"),
        check_vma=False,
    )
```
